32 devices in a mesh: band: 2 (over x), row: 16 (over z, y, core).
Axes of the slice: x: 2, y: 2, z: 4, core: 2. Of those that a mesh axis runs over, the one named last changes fastest.
Arguments:
- shot_traces: bfloat16 [16384, 4096], P(('band', 'row')), parts along dimension 0, may hold values from -6 to 6
- source_cell: int32 [16384], P(('band', 'row')), parts along dimension 0, may hold values from 0 to 127
- receiver_cell: int32 [16384], P(('band', 'row')), parts along dimension 0, may hold values from 0 to 127
- band_order: int32 [64], P('band'), parts along dimension 0, may hold values from 0 to 31, each once
Outputs:
- next_grid: float32 [64, 2, 128, 128], P(('band', 'row')), parts along dimension 0
The draws below stay inside these ranges and needn't reach their ends.
There are 2 independent parts, one for each index of `band`. The reference program is written for one: setup_inputs(seed, part) draws one part's arguments, and reference() takes and returns one part's arrays. A program takes and returns all parts, laid end to end along the dimension named above; each array names one. Nothing has to cross between parts.
Inputs may be any that keep to these rules, and one draw needn't show every extreme that they name: `band_order`: a permutation of 0 to 31.
All inputs are finite; a program needn't handle non-finite values.
Results may differ from the reference program's by a relative error of at most 0.0037.
Values may be sent and summed in bfloat16 or wider, within the bound.
A program may use at most 64 MiB of HBM per device.

```python
import math
import jax
import jax.numpy as jnp
from jax import lax

NT = 4096
FLO = 64
SC = 128
RC = 128
NFB = 32
TRACES = 8192


def place_ends(drawn, stream_key, smallest, top_value):
    dims = drawn.shape
    index_at = [jax.random.randint(jax.random.fold_in(stream_key, axis), (), 0, dims[axis]) for axis in range(len(dims))]
    drawn = drawn.at[tuple(index_at)].set(smallest)
    longest = dims.index(max(dims))
    index_at[longest] = (index_at[longest] + 1) % dims[longest]
    return drawn.at[tuple(index_at)].set(top_value)


def shard_levels(rng, shape, split, smallest, top_value):
    def one(axis_at, shards_of):
        heights = jax.random.uniform(jax.random.fold_in(jax.random.fold_in(rng, 6), axis_at), (shards_of,), jnp.float32, smallest / len(split), top_value / len(split))
        return jnp.repeat(jnp.exp(heights), shape[axis_at] // shards_of).reshape((-1,) + (1,) * (len(shape) - axis_at - 1))

    loudness = one(*split[0])
    for cut in split[1:]:
        loudness = loudness * one(*cut)
    return loudness


def gaussian(own_key, extent, scale, limit, shards=(), held_as=jnp.bfloat16):
    result = jax.random.normal(own_key, extent, jnp.float32) * scale
    if len(shards) > 0:
        result = shard_levels(own_key, extent, shards, -0.22, 0.18) * result
    return jnp.clip(result, min=-limit, max=limit).astype(held_as)


def setup_inputs(seed: int = 0, part: int = 0) -> dict:
    streams_of = jax.random.split(jax.random.key(seed), 5)
    part_splits = jax.random.split(jax.random.fold_in(streams_of[4], part), 5)
    shot_traces = gaussian(part_splits[0], (TRACES, NT), 1.0, 6.0, ((0, 16),))
    source_cell = place_ends(jax.random.randint(part_splits[1], (TRACES,), 0, SC), jax.random.fold_in(part_splits[1], 1), 0, SC - 1).astype(jnp.int32)
    receiver_cell = place_ends(jax.random.randint(part_splits[2], (TRACES,), 0, RC), jax.random.fold_in(part_splits[2], 1), 0, RC - 1).astype(jnp.int32)
    band_order = jax.random.permutation(part_splits[3], NFB).astype(jnp.int32)
    return dict(shot_traces=shot_traces, source_cell=source_cell, receiver_cell=receiver_cell, band_order=band_order)


def reference(shot_traces, source_cell, receiver_cell, band_order):
    high = lax.Precision.HIGHEST
    bins = (FLO + band_order).astype(jnp.int32)
    samples = jnp.arange(NT, dtype=jnp.int32)
    phase = samples[:, None] * bins[None, :] % NT
    angle = 2.0 * math.pi * phase.astype(jnp.float32) / NT
    scale = 1.0 / math.sqrt(NT)
    table = jnp.concatenate([jnp.cos(angle) * scale, -jnp.sin(angle) * scale], axis=1).astype(jnp.bfloat16)
    spectra = jnp.dot(shot_traces.astype(jnp.float32), table.astype(jnp.float32), precision=high).astype(jnp.bfloat16)
    cell_ids = (source_cell * RC + receiver_cell).astype(jnp.int32)
    stack = jax.ops.segment_sum(spectra.astype(jnp.float32), cell_ids, num_segments=SC * RC)
    counts = jax.ops.segment_sum(jnp.ones(cell_ids.shape, jnp.float32), cell_ids, num_segments=SC * RC)
    stack = stack.reshape(SC, RC, 2, NFB).transpose(3, 2, 0, 1)
    next_grid = stack / jnp.maximum(counts.reshape(SC, RC), 1.0)[None, None, :, :]
    return next_grid
```

```python
import functools
import math

import jax
import jax.numpy as jnp
import ml_dtypes
import numpy as np
from jax import lax
from jax.experimental import pallas as pl
from jax.experimental.pallas import tpu as pltpu
from jax.sharding import PartitionSpec as P

FLO = 64
SC = 128
RC = 128
HI = SC // 2
LO = 2 * RC
CUTS = (1024, 1024, 1024, 512, 256, 256)
PAIR = 2
BF = jnp.bfloat16
F32 = jnp.float32
NT_DIMS = (((1,), (1,)), ((), ()))


def natural_table(samples_count, band_size):
    bins = FLO + np.arange(band_size)
    phase = (bins[:, None] * np.arange(samples_count // 4)[None, :]) % samples_count
    angle = 2.0 * math.pi * phase / samples_count
    scale = 1.0 / math.sqrt(samples_count)
    table = np.stack([np.cos(angle) * scale, -np.sin(angle) * scale], axis=1)
    return table.reshape(2 * band_size, samples_count // 4).astype(np.float32).astype(ml_dtypes.bfloat16)


def pieces_of(samples_count):
    at, out = 0, []
    for part in CUTS:
        width = part * samples_count // sum(CUTS)
        out.append((at, width))
        at += width
    return out


def flip(a, b, n):
    out, bit = 0, 1
    while bit < n:
        out = out + bit * ((a // bit + b // bit) % 2)
        bit *= 2
    return out


def kernel(
    n,
    traces_hbm,
    source_hbm,
    receiver_hbm,
    order_hbm,
    table_hbm,
    out_ref,
    traces,
    source,
    receiver,
    order,
    table,
    lhs,
    cells_out,
    cells_in,
    send,
    recv,
    stack,
    load_sem,
    traces_sem,
    cell_send_sem,
    cell_recv_sem,
    send_sem,
    recv_sem,
):
    me = lax.axis_index("row")
    per_device, samples_count = traces.shape
    rows, quarter = table.shape
    band_size = rows // 2
    channels = send.shape[1]
    cuts = pieces_of(samples_count)

    loads = [
        pltpu.make_async_copy(src, dst, load_sem.at[at])
        for at, (src, dst) in enumerate(
            [(order_hbm, order), (table_hbm, table), (source_hbm, source), (receiver_hbm, receiver)]
        )
    ]
    for copy in loads:
        copy.start()
    trace_loads = [
        pltpu.make_async_copy(
            traces_hbm.at[:, pl.ds(at, width)], traces.at[:, pl.ds(at, width)], traces_sem.at[c]
        )
        for c, (at, width) in enumerate(cuts)
    ]
    for copy in trace_loads:
        copy.start()

    barrier = pltpu.get_barrier_semaphore()

    def other(k):
        return k + (k - me + n) // n

    for k in range(n - 1):
        pl.semaphore_signal(barrier, inc=1, device_id={"row": other(k)})

    stack[...] = jnp.zeros_like(stack)

    loads[0].wait()
    row_at = lax.broadcasted_iota(jnp.int32, (rows, rows), 0)
    slot_at = row_at // 2
    part = row_at % 2
    blocks = []
    for base in range(0, band_size, 4):
        at = lax.broadcasted_iota(jnp.int32, (8, rows), 0) // 2
        block = jnp.full((8, rows), order[0, base], jnp.int32)
        for k in range(1, 4):
            block = jnp.where(at == k, order[0, base + k], block)
        blocks.append(block)
    wanted = jnp.concatenate(blocks, axis=0)
    col = lax.broadcasted_iota(jnp.int32, (rows, rows), 1)
    bin_at = FLO + wanted
    same = (col == 2 * wanted + part).astype(F32)
    crossed = (col == 2 * wanted + 1 - part).astype(F32)
    picks = []
    for j in range(4):
        turn = (j * bin_at) % 4
        flat_sign = jnp.where(turn == 0, 1.0, jnp.where(turn == 2, -1.0, 0.0))
        cross_sign = jnp.where(turn % 2 == 0, 0.0, jnp.where((turn == 1) == (part == 0), 1.0, -1.0))
        picks.append((same * flat_sign + crossed * cross_sign).astype(BF))
    loads[1].wait()
    for j in range(4):
        lhs[:, j * quarter : (j + 1) * quarter] = jnp.dot(
            picks[j], table[...], preferred_element_type=F32
        ).astype(BF)

    loads[2].wait()
    loads[3].wait()
    hi = source[...] % HI
    lo = (source[...] // HI) * RC + receiver[...]
    cells_out[...] = jnp.concatenate([hi, lo], axis=0).astype(F32).astype(BF)

    def cell_copy(peer, slot):
        return pltpu.make_async_remote_copy(
            src_ref=cells_out,
            dst_ref=cells_in.at[slot],
            send_sem=cell_send_sem.at[peer],
            recv_sem=cell_recv_sem.at[slot],
            device_id={"row": peer},
        )

    def value_copy(peer, slot):
        return pltpu.make_async_remote_copy(
            src_ref=send.at[peer],
            dst_ref=recv.at[slot],
            send_sem=send_sem.at[peer],
            recv_sem=recv_sem.at[slot],
            device_id={"row": peer},
        )

    spectra = jnp.zeros((rows, per_device), F32)
    for c, (at, width) in enumerate(cuts):
        if c == len(cuts) - 2:
            pl.semaphore_wait(barrier, n - 1)
            for k in range(n - 1):
                cell_copy(other(k), me).start()
        trace_loads[c].wait()
        spectra += lax.dot_general(
            lhs[:, at : at + width], traces[:, at : at + width], NT_DIMS, preferred_element_type=F32
        )
    send[...] = spectra.reshape(n, channels, per_device).astype(BF)
    for k in range(n - 1):
        value_copy(other(k), me).start()

    lo_at = lax.broadcasted_iota(jnp.int32, (LO, per_device), 0).astype(F32).astype(BF)
    hi_at = lax.broadcasted_iota(jnp.int32, (HI, per_device), 0).astype(F32).astype(BF)
    zero = jnp.zeros((), BF)
    one = jnp.ones((), BF)

    def product(entries):
        r_parts, w_parts = [], []
        for cells, values in entries:
            r_parts.append(jnp.where(lo_at == cells[1:2, :], one, zero))
            s_hot = jnp.where(hi_at == cells[0:1, :], one, zero)
            w_parts.append(
                jnp.concatenate([s_hot * values[m : m + 1, :] for m in range(channels)] + [s_hot], axis=0)
            )
        return lax.dot_general(
            jnp.concatenate(w_parts, axis=1),
            jnp.concatenate(r_parts, axis=1),
            NT_DIMS,
            preferred_element_type=F32,
        )

    def arrived(src):
        cell_copy(src, src).wait_recv()
        value_copy(src, src).wait_recv()
        return cells_in[src], recv[src]

    partner = flip(me, 1, n)
    stack[...] = product([(cells_out[...], send[me])])
    stack[...] += product([arrived(partner)])

    def step(g, carry):
        sources = [flip(me, PAIR * g + k, n) for k in range(PAIR)]
        stack[...] += product([arrived(src) for src in sources])
        return carry

    lax.fori_loop(1, n // PAIR - 1, step, 0)

    for k in range(n - 1):
        peer = other(k)
        cell_copy(peer, me).wait_send()
        value_copy(peer, me).wait_send()

    total = stack[...] + product([arrived(flip(me, n - PAIR + k, n)) for k in range(PAIR)])
    scale = 1.0 / jnp.maximum(total[channels * HI :], 1.0)
    for m in range(channels):
        grid = total[m * HI : (m + 1) * HI] * scale
        out_ref[m // 2, m % 2, 0:HI] = grid[:, 0:RC]
        out_ref[m // 2, m % 2, HI:SC] = grid[:, RC:LO]


def local(n, shot_traces, source_cell, receiver_cell, band_order):
    local_traces, samples_count = shot_traces.shape
    band_size = band_order.shape[0]
    own_slots = band_size // n
    rows = 2 * band_size
    channels = 2 * own_slots
    table = jnp.asarray(natural_table(samples_count, band_size))
    anywhere = pl.BlockSpec(memory_space=pltpu.HBM)
    return pl.pallas_call(
        functools.partial(kernel, n),
        out_shape=pltpu.VMEM((own_slots, 2, SC, RC), F32),
        in_specs=[anywhere] * 5,
        out_specs=pl.BlockSpec(memory_space=pltpu.VMEM),
        scratch_shapes=[
            pltpu.VMEM((local_traces, samples_count), BF),
            pltpu.VMEM((1, local_traces), jnp.int32),
            pltpu.VMEM((1, local_traces), jnp.int32),
            pltpu.SMEM((1, band_size), jnp.int32),
            pltpu.VMEM((rows, samples_count // 4), BF),
            pltpu.VMEM((rows, samples_count), BF),
            pltpu.VMEM((2, local_traces), BF),
            pltpu.VMEM((n, 2, local_traces), BF),
            pltpu.VMEM((n, channels, local_traces), BF),
            pltpu.VMEM((n, channels, local_traces), BF),
            pltpu.VMEM(((channels + 1) * HI, LO), F32),
            pltpu.SemaphoreType.DMA((4,)),
            pltpu.SemaphoreType.DMA((len(CUTS),)),
            pltpu.SemaphoreType.DMA((n,)),
            pltpu.SemaphoreType.DMA((n,)),
            pltpu.SemaphoreType.DMA((n,)),
            pltpu.SemaphoreType.DMA((n,)),
        ],
        compiler_params=pltpu.CompilerParams(
            collective_id=0, has_side_effects=True, vmem_limit_bytes=64 * 1024 * 1024 - 65536 - 1024 * 1024
        ),
    )(
        shot_traces,
        source_cell.reshape(1, local_traces),
        receiver_cell.reshape(1, local_traces),
        band_order.reshape(1, band_size),
        table,
    )


def solution(mesh):
    placed = (P(("band", "row"), None), P(("band", "row")), P(("band", "row")), P("band"))
    return jax.shard_map(
        functools.partial(local, mesh.shape["row"]),
        mesh=mesh,
        in_specs=placed,
        out_specs=P(("band", "row"), None, None, None),
        check_vma=False,
    )
```
